32 devices in a mesh: clip: 2 (over x), tm: 16 (over z, y, core).
Axes of the slice: x: 2, y: 2, z: 4, core: 2. Of those that a mesh axis runs over, the one named last changes fastest.
Arguments:
- frames: bfloat16 [64, 1024, 256], P('tm', 'clip'), parts along dimension 1, may hold values from -6 to 6
- gain_one: float32 [256], replicated, may hold values from 0.25 to 1.75
- conv_one: bfloat16 [3, 3, 3, 256, 256], replicated, may hold values from -0.078125 to 0.078125
- gain_two: float32 [256], replicated, may hold values from 0.25 to 1.75
- conv_two: bfloat16 [3, 3, 3, 256, 256], replicated, may hold values from -0.078125 to 0.078125
- out_weight: bfloat16 [256, 256], replicated, may hold values from -0.375 to 0.375
Outputs:
- latent: bfloat16 [64, 1024, 256], P(None, ('clip', 'tm')), parts along dimension 1
The draws below stay inside these ranges and needn't reach their ends.
There are 2 independent parts, one for each index of `clip`. The reference program is written for one: setup_inputs(seed, part) draws one part's arguments, and reference() takes and returns one part's arrays. A program takes and returns all parts, laid end to end along the dimension named above; an argument that names none is the same for every part. Nothing has to cross between parts.
All inputs are finite; a program needn't handle non-finite values.
Results may differ from the reference program's by a relative error of at most 0.0065.
Values may be sent and summed in bfloat16 or wider, within the bound.
A program may use at most 192 MiB of HBM per device.

```python
import jax
import jax.numpy as jnp
from jax import lax

C = 256
ROWS = 4
COLS = 128
CELLS = 512
FRAMES = 64


def levels(rng, dims, split, low, largest):
    def one(axis_at, shards_of):
        steps = jax.random.uniform(jax.random.fold_in(jax.random.fold_in(rng, 6), axis_at), (shards_of,), jnp.float32, low / len(split), largest / len(split))
        return jnp.repeat(jnp.exp(steps), dims[axis_at] // shards_of).reshape((-1,) + (1,) * (len(dims) - axis_at - 1))

    factor_of = one(*split[0])
    for cut in split[1:]:
        factor_of = factor_of * one(*cut)
    return factor_of


def bell_draw(stream_key, shape, width, limit, cuts=(), kind=jnp.bfloat16):
    values = width * jax.random.normal(stream_key, shape, jnp.float32)
    if cuts:
        values = values * levels(stream_key, shape, cuts, -0.22, 0.18)
    return jnp.clip(values, -limit, limit).astype(kind)


def setup_inputs(seed: int = 0, part: int = 0) -> dict:
    arg_keys = jax.random.split(jax.random.key(seed), 7)
    part_splits = jax.random.split(jax.random.fold_in(arg_keys[6], part), 7)
    return {
        "frames": bell_draw(part_splits[0], (FRAMES, CELLS, C), 1.0, 6.0, ((0, 16),)),
        "gain_one": jnp.clip(1.0 + 0.15 * jax.random.normal(arg_keys[1], (C,), jnp.float32), 0.25, 1.75),
        "conv_one": bell_draw(arg_keys[2], (3, 3, 3, C, C), (27 * C) ** -0.5, 0.078125),
        "gain_two": jnp.clip(1.0 + 0.15 * jax.random.normal(arg_keys[3], (C,), jnp.float32), 0.25, 1.75),
        "conv_two": bell_draw(arg_keys[4], (3, 3, 3, C, C), (27 * C) ** -0.5, 0.078125),
        "out_weight": bell_draw(arg_keys[5], (C, C), C ** -0.5, 0.375),
    }


def norm_act(x, gain):
    values = x.astype(jnp.float32)
    scale = lax.rsqrt(lax.optimization_barrier(jnp.mean(values * values, axis=-1, keepdims=True)) + 1e-06)
    return jax.nn.silu(values * scale * gain).astype(jnp.bfloat16)

def causal_conv(act, kernel):
    frame_count = act.shape[0]
    channels = act.shape[-1]
    grid = act.reshape(frame_count, ROWS, COLS, channels)
    padded = jnp.pad(grid, ((2, 0), (1, 1), (1, 1), (0, 0)))
    total = jnp.zeros((frame_count * ROWS * COLS, channels), jnp.float32)
    for tap_t in range(3):
        for tap_r in range(3):
            for tap_c in range(3):
                slab = padded[tap_t:tap_t + frame_count, tap_r:tap_r + ROWS, tap_c:tap_c + COLS, :]
                total = total + jnp.dot(slab.reshape(-1, channels), kernel[tap_t, tap_r, tap_c], preferred_element_type=jnp.float32)
    return total.reshape(frame_count, ROWS * COLS, channels)

def block(x, gain, kernel):
    act = norm_act(x, gain)
    return (x.astype(jnp.float32) + causal_conv(act, kernel)).astype(jnp.bfloat16)

def reference(frames, gain_one, conv_one, gain_two, conv_two, out_weight):
    first = block(frames, gain_one, conv_one)
    second = block(first, gain_two, conv_two)
    channels = second.shape[-1]
    latent = jnp.dot(second.reshape(-1, channels), out_weight, preferred_element_type=jnp.float32)
    return latent.reshape(second.shape).astype(jnp.bfloat16)
```

```python
import functools

import jax
import jax.numpy as jnp
from jax import lax
from jax.experimental import pallas as pl
from jax.experimental.pallas import tpu as pltpu
from jax.sharding import PartitionSpec as P

ROWS = 4
COLS = 128
MESH = pl.DeviceIdType.MESH


def norm_act(x, gain):
    values = x.astype(jnp.float32)
    scale = lax.rsqrt(jnp.mean(values * values, axis=-1, keepdims=True) + 1e-06)
    scaled = values * scale * gain
    return scaled * (0.5 * jnp.tanh(0.5 * scaled) + 0.5)


def store_shifted(acts, frame, row, act):
    channels = act.shape[-1]
    place = lax.broadcasted_iota(jnp.int32, act.shape, 0)
    before = jnp.where(place == 0, 0.0, pltpu.roll(act, 1, 0))
    after = jnp.where(place == COLS - 1, 0.0, pltpu.roll(act, COLS - 1, 0))
    acts[frame, row, :, :channels] = before.astype(jnp.bfloat16)
    acts[frame, row, :, channels : 2 * channels] = act.astype(jnp.bfloat16)
    acts[frame, row, :, 2 * channels :] = after.astype(jnp.bfloat16)


def conv_row(acts, kernel, frame, row):
    total = None
    for tap_t in range(3):
        for tap_r in range(3):
            source = row + tap_r - 1
            if 0 <= source < ROWS:
                window = acts[frame + tap_t : frame + tap_t + 2, source]
                part = jnp.dot(
                    window.reshape(2 * COLS, window.shape[-1]),
                    kernel[tap_t * 3 + tap_r],
                    preferred_element_type=jnp.float32,
                )
                total = part if total is None else total + part
    return total


def fused(
    n,
    frames_ref,
    gain_one,
    conv_one,
    gain_two,
    conv_two,
    out_weight,
    out_ref,
    frames,
    halo_one,
    halo_two,
    edge_two,
    kernel_one,
    kernel_two,
    acts_one,
    acts_two,
    first,
    result,
    load_sems,
    halo_send,
    halo_recv,
    edge_send,
    edge_recv,
    out_send,
    out_recv,
    own_sem,
):
    me = lax.axis_index("tm")
    count = frames.shape[0]
    channels = frames.shape[-1]
    owned = result.shape[2]
    per_row = COLS // owned
    earlier = me - 1
    later = me + 1

    loads = [
        pltpu.make_async_copy(frames_ref, frames, load_sems.at[0]),
        pltpu.make_async_copy(conv_one, kernel_one, load_sems.at[1]),
        pltpu.make_async_copy(conv_two, kernel_two, load_sems.at[2]),
    ]
    for load in loads:
        load.start()

    barrier = pltpu.get_barrier_semaphore()

    @pl.loop(1, n)
    def _(step):
        pl.semaphore_signal(
            barrier, inc=1, device_id={"tm": lax.rem(me + step, n)}, device_id_type=MESH
        )

    loads[0].wait()

    @pl.loop(0, count * ROWS)
    def _(index):
        frame = index // ROWS
        row = index % ROWS
        act = norm_act(frames[frame, row], gain_one[...])
        store_shifted(acts_one, frame + 2, row, act)

    pl.semaphore_wait(barrier, n - 1)

    halo_copy = pltpu.make_async_remote_copy(
        src_ref=frames_ref.at[pl.ds(count - 2, 2)],
        dst_ref=halo_one,
        send_sem=halo_send,
        recv_sem=halo_recv,
        device_id={"tm": lax.rem(later, n)},
        device_id_type=MESH,
    )

    def edge_copy(row):
        return pltpu.make_async_remote_copy(
            src_ref=edge_two.at[row],
            dst_ref=halo_two.at[row],
            send_sem=edge_send.at[row],
            recv_sem=edge_recv.at[row],
            device_id={"tm": lax.rem(later, n)},
            device_id_type=MESH,
        )

    @pl.when(later < n)
    def _():
        halo_copy.start()

    loads[1].wait()

    def first_pair(frame):
        for row in range(ROWS):
            conv = conv_row(acts_one, kernel_one, frame, row).reshape(2, COLS, channels)
            for at in range(2):
                value = (frames[frame + at, row].astype(jnp.float32) + conv[at]).astype(
                    jnp.bfloat16
                )
                first[frame + at, row] = value
                act = norm_act(value, gain_two[...])
                store_shifted(acts_two, frame + at + 2, row, act)
                if frame == count - 2:
                    edge_two[row, at] = act.astype(jnp.bfloat16)
            if frame == count - 2:

                @pl.when(later < n)
                def _():
                    edge_copy(row).start()

    def second_pair(frame):
        for row in range(ROWS):
            conv = conv_row(acts_two, kernel_two, frame, row).reshape(2, COLS, channels)
            value = (first[frame : frame + 2, row].astype(jnp.float32) + conv).astype(jnp.bfloat16)
            latent = jnp.dot(
                value.reshape(2 * COLS, channels),
                out_weight[...],
                preferred_element_type=jnp.float32,
            ).astype(jnp.bfloat16)
            for at in range(2):
                for index in range(per_row):
                    begin = at * COLS + index * owned
                    result[row * per_row + index, frame + at] = latent[begin : begin + owned]

            @pl.loop(0, per_row)
            def _(index):
                owner = row * per_row + index

                @pl.when(owner != me)
                def _():
                    pltpu.make_async_remote_copy(
                        src_ref=result.at[owner, pl.ds(frame, 2)],
                        dst_ref=out_ref.at[pl.ds(me * count + frame, 2)],
                        send_sem=out_send,
                        recv_sem=out_recv,
                        device_id={"tm": owner},
                        device_id_type=MESH,
                    ).start()

    for frame in reversed(range(2, count, 2)):
        first_pair(frame)

    @pl.when(me > 0)
    def _():
        halo_copy.wait_recv()

        @pl.loop(0, 2 * ROWS)
        def _(index):
            frame = index // ROWS
            row = index % ROWS
            act = norm_act(halo_one[frame, row], gain_one[...])
            store_shifted(acts_one, frame, row, act)

    @pl.when(me == 0)
    def _():
        @pl.loop(0, 2 * ROWS)
        def _(index):
            blank = jnp.zeros((COLS, acts_one.shape[-1]), jnp.bfloat16)
            acts_one[index // ROWS, index % ROWS] = blank
            acts_two[index // ROWS, index % ROWS] = blank

    first_pair(0)
    loads[2].wait()
    for frame in reversed(range(2, count, 2)):
        second_pair(frame)

    @pl.when(me > 0)
    def _():
        for row in range(ROWS):
            edge_copy(row).wait_recv()
            for at in range(2):
                store_shifted(acts_two, at, row, halo_two[row, at].astype(jnp.float32))

    second_pair(0)
    own = pltpu.make_async_copy(result.at[me], out_ref.at[pl.ds(me * count, count)], own_sem)
    own.start()

    @pl.when(later < n)
    def _():
        halo_copy.wait_send()
        for row in range(ROWS):
            edge_copy(row).wait_send()

    others = out_ref.at[pl.ds(0, (n - 1) * count)]
    sent = result.at[pl.ds(0, n - 1)]
    pltpu.make_async_copy(sent, sent, out_send).wait()
    pltpu.make_async_copy(others, others, out_recv).wait()
    own.wait()


def body(n, frames, gain_one, conv_one, gain_two, conv_two, out_weight):
    count, cells, channels = frames.shape
    owned = cells // n
    grid = (count, ROWS, COLS, channels)
    taps = (9, 3 * channels, channels)
    half = jnp.bfloat16
    hbm = pl.BlockSpec(memory_space=pl.ANY)
    vmem = pl.BlockSpec(memory_space=pltpu.VMEM)
    return pl.pallas_call(
        functools.partial(fused, n),
        out_shape=jax.ShapeDtypeStruct((n * count, owned, channels), half),
        in_specs=[hbm, vmem, hbm, vmem, hbm, vmem],
        out_specs=hbm,
        scratch_shapes=[
            pltpu.VMEM(grid, half),
            pltpu.VMEM((2, ROWS, COLS, channels), half),
            pltpu.VMEM((ROWS, 2, COLS, channels), half),
            pltpu.VMEM((ROWS, 2, COLS, channels), half),
            pltpu.VMEM(taps, half),
            pltpu.VMEM(taps, half),
            pltpu.VMEM((count + 2, ROWS, COLS, 3 * channels), half),
            pltpu.VMEM((count + 2, ROWS, COLS, 3 * channels), half),
            pltpu.VMEM(grid, half),
            pltpu.VMEM((n, count, owned, channels), half),
            pltpu.SemaphoreType.DMA((3,)),
            pltpu.SemaphoreType.DMA,
            pltpu.SemaphoreType.DMA,
            pltpu.SemaphoreType.DMA((ROWS,)),
            pltpu.SemaphoreType.DMA((ROWS,)),
            pltpu.SemaphoreType.DMA,
            pltpu.SemaphoreType.DMA,
            pltpu.SemaphoreType.DMA,
        ],
        compiler_params=pltpu.CompilerParams(collective_id=0, has_side_effects=True),
    )(
        frames.reshape(grid),
        gain_one.reshape(1, channels),
        conv_one.reshape(taps),
        gain_two.reshape(1, channels),
        conv_two.reshape(taps),
        out_weight,
    )


def solution(mesh):
    placed = (P("tm", "clip", None), P(), P(), P(), P(), P())
    return jax.shard_map(
        functools.partial(body, mesh.shape["tm"]),
        mesh=mesh,
        in_specs=placed,
        out_specs=P(None, ("clip", "tm"), None),
        check_vma=False,
    )
```

```python
import functools

import jax
import jax.numpy as jnp
from jax import lax
from jax.experimental import pallas as pl
from jax.experimental.pallas import tpu as pltpu
from jax.sharding import PartitionSpec as P

ROWS = 4
COLS = 128
MESH = pl.DeviceIdType.MESH


def norm_act(x, gain):
    values = x.astype(jnp.float32)
    scale = lax.rsqrt(jnp.mean(values * values, axis=-1, keepdims=True) + 1e-06)
    scaled = values * scale * gain
    return scaled * (0.5 * jnp.tanh(0.5 * scaled) + 0.5)


def store_shifted(acts, frame, row, act):
    channels = act.shape[-1]
    place = lax.broadcasted_iota(jnp.int32, act.shape, 0)
    before = jnp.where(place == 0, 0.0, pltpu.roll(act, 1, 0))
    after = jnp.where(place == COLS - 1, 0.0, pltpu.roll(act, COLS - 1, 0))
    acts[frame, row, :, :channels] = before.astype(jnp.bfloat16)
    acts[frame, row, :, channels : 2 * channels] = act.astype(jnp.bfloat16)
    acts[frame, row, :, 2 * channels :] = after.astype(jnp.bfloat16)


def conv_row(acts, kernel, frame, source, tap, rows):
    total = None
    for tap_t in range(3):
        for at in range(rows):
            window = acts[pl.ds(frame + tap_t, 2), source + at]
            part = jnp.dot(
                window.reshape(2 * COLS, window.shape[-1]),
                kernel[tap_t * 3 + tap + at],
                preferred_element_type=jnp.float32,
            )
            total = part if total is None else total + part
    return total.reshape(2, COLS, total.shape[-1])


def both_rows(acts, kernel, frame, half):
    border = conv_row(acts, kernel, frame, 2 * half, 1 - half, 2)
    inner = conv_row(acts, kernel, frame, half, 0, 3)
    return (((ROWS - 1) * half, border), (1 + half, inner))


def fused(
    n,
    frames_ref,
    gain_one,
    conv_one,
    gain_two,
    conv_two,
    out_weight,
    out_ref,
    frames,
    halo_one,
    halo_two,
    edge_two,
    kernel_one,
    kernel_two,
    project,
    acts_one,
    acts_two,
    first,
    result,
    load_sems,
    halo_send,
    halo_recv,
    edge_send,
    edge_recv,
    out_send,
    out_recv,
    own_sem,
):
    me = lax.axis_index("tm")
    count = frames.shape[0]
    channels = frames.shape[-1]
    owned = result.shape[2]
    per_row = COLS // owned
    earlier = me - 1
    later = me + 1

    loads = [pltpu.make_async_copy(frames_ref, frames, load_sems.at[0])]
    for source, target in ((conv_one, kernel_one), (conv_two, kernel_two)):
        for tap in range(9):
            sem = load_sems.at[len(loads)]
            loads.append(pltpu.make_async_copy(source.at[tap], target.at[tap], sem))
    loads.append(pltpu.make_async_copy(out_weight, project, load_sems.at[19]))
    for load in loads[:10]:
        load.start()

    barrier = pltpu.get_barrier_semaphore()

    @pl.loop(1, n)
    def _(step):
        pl.semaphore_signal(
            barrier, inc=1, device_id={"tm": lax.rem(me + step, n)}, device_id_type=MESH
        )

    loads[0].wait()

    @pl.loop(0, count * ROWS)
    def _(index):
        frame = index // ROWS
        row = index % ROWS
        act = norm_act(frames[frame, row], gain_one[...])
        store_shifted(acts_one, frame + 2, row, act)

    pl.semaphore_wait(barrier, n - 1)

    halo_copy = pltpu.make_async_remote_copy(
        src_ref=frames_ref.at[pl.ds(count - 2, 2)],
        dst_ref=halo_one,
        send_sem=halo_send,
        recv_sem=halo_recv,
        device_id={"tm": lax.rem(later, n)},
        device_id_type=MESH,
    )

    def edge_copy(row):
        return pltpu.make_async_remote_copy(
            src_ref=edge_two.at[row],
            dst_ref=halo_two.at[row],
            send_sem=edge_send.at[row],
            recv_sem=edge_recv.at[row],
            device_id={"tm": lax.rem(later, n)},
            device_id_type=MESH,
        )

    @pl.when(later < n)
    def _():
        halo_copy.start()

    for load in loads[1:10]:
        load.wait()
    for load in loads[10:]:
        load.start()

    halves = ROWS // 2
    steps = (count // 2) * halves

    @pl.loop(0, steps)
    def _(step):
        frame = count - 2 - 2 * (step // halves)
        half = step % halves

        @pl.when((step == steps - halves) & (me > 0))
        def _():
            halo_copy.wait_recv()

            @pl.loop(0, 2 * ROWS)
            def _(index):
                at = index // ROWS
                row = index % ROWS
                store_shifted(acts_one, at, row, norm_act(halo_one[at, row], gain_one[...]))

        @pl.when((step == steps - halves) & (me == 0))
        def _():
            @pl.loop(0, 2 * ROWS)
            def _(index):
                blank = jnp.zeros((COLS, acts_one.shape[-1]), jnp.bfloat16)
                acts_one[index // ROWS, index % ROWS] = blank
                acts_two[index // ROWS, index % ROWS] = blank

        for row, conv in both_rows(acts_one, kernel_one, frame, half):
            for at in range(2):
                value = (frames[frame + at, row].astype(jnp.float32) + conv[at]).astype(
                    jnp.bfloat16
                )
                first[frame + at, row] = value
                store_shifted(acts_two, frame + at + 2, row, norm_act(value, gain_two[...]))

        @pl.when((step < halves) & (later < n))
        def _():
            for row in ((ROWS - 1) * half, 1 + half):
                for at in range(2):
                    edge_two[row, at] = acts_two[count + at, row, :, channels : 2 * channels]
                edge_copy(row).start()

    for load in loads[10:]:
        load.wait()

    @pl.loop(0, steps)
    def _(step):
        frame = count - 2 - 2 * (step // halves)
        half = step % halves

        @pl.when((step == steps - halves) & (me > 0))
        def _():
            @pl.loop(0, ROWS)
            def _(row):
                edge_copy(row).wait_recv()
                for at in range(2):
                    store_shifted(acts_two, at, row, halo_two[row, at].astype(jnp.float32))

        for row, conv in both_rows(acts_two, kernel_two, frame, half):
            value = (first[pl.ds(frame, 2), row].astype(jnp.float32) + conv).astype(jnp.bfloat16)
            latent = jnp.dot(
                value.reshape(2 * COLS, channels),
                project[...],
                preferred_element_type=jnp.float32,
            ).astype(jnp.bfloat16)
            for at in range(2):
                for index in range(per_row):
                    begin = at * COLS + index * owned
                    result[row * per_row + index, frame + at] = latent[begin : begin + owned]

        for row in ((ROWS - 1) * half, 1 + half):

            @pl.loop(0, per_row)
            def _(index):
                owner = row * per_row + index

                @pl.when(owner != me)
                def _():
                    pltpu.make_async_remote_copy(
                        src_ref=result.at[owner, pl.ds(frame, 2)],
                        dst_ref=out_ref.at[pl.ds(me * count + frame, 2)],
                        send_sem=out_send,
                        recv_sem=out_recv,
                        device_id={"tm": owner},
                        device_id_type=MESH,
                    ).start()

    own = pltpu.make_async_copy(result.at[me], out_ref.at[pl.ds(me * count, count)], own_sem)
    own.start()

    @pl.when(later < n)
    def _():
        halo_copy.wait_send()
        for row in range(ROWS):
            edge_copy(row).wait_send()

    others = out_ref.at[pl.ds(0, (n - 1) * count)]
    sent = result.at[pl.ds(0, n - 1)]
    pltpu.make_async_copy(sent, sent, out_send).wait()
    pltpu.make_async_copy(others, others, out_recv).wait()
    own.wait()


def body(n, frames, gain_one, conv_one, gain_two, conv_two, out_weight):
    count, cells, channels = frames.shape
    owned = cells // n
    grid = (count, ROWS, COLS, channels)
    taps = (9, 3 * channels, channels)
    half = jnp.bfloat16
    hbm = pl.BlockSpec(memory_space=pl.ANY)
    vmem = pl.BlockSpec(memory_space=pltpu.VMEM)
    return pl.pallas_call(
        functools.partial(fused, n),
        out_shape=jax.ShapeDtypeStruct((n * count, owned, channels), half),
        in_specs=[hbm, vmem, hbm, vmem, hbm, hbm],
        out_specs=hbm,
        scratch_shapes=[
            pltpu.VMEM(grid, half),
            pltpu.VMEM((2, ROWS, COLS, channels), half),
            pltpu.VMEM((ROWS, 2, COLS, channels), half),
            pltpu.VMEM((ROWS, 2, COLS, channels), half),
            pltpu.VMEM(taps, half),
            pltpu.VMEM(taps, half),
            pltpu.VMEM((channels, channels), half),
            pltpu.VMEM((count + 2, ROWS, COLS, 3 * channels), half),
            pltpu.VMEM((count + 2, ROWS, COLS, 3 * channels), half),
            pltpu.VMEM(grid, half),
            pltpu.VMEM((n, count, owned, channels), half),
            pltpu.SemaphoreType.DMA((20,)),
            pltpu.SemaphoreType.DMA,
            pltpu.SemaphoreType.DMA,
            pltpu.SemaphoreType.DMA((ROWS,)),
            pltpu.SemaphoreType.DMA((ROWS,)),
            pltpu.SemaphoreType.DMA,
            pltpu.SemaphoreType.DMA,
            pltpu.SemaphoreType.DMA,
        ],
        compiler_params=pltpu.CompilerParams(collective_id=0, has_side_effects=True),
    )(
        frames.reshape(grid),
        gain_one.reshape(1, channels),
        conv_one.reshape(taps),
        gain_two.reshape(1, channels),
        conv_two.reshape(taps),
        out_weight,
    )


def solution(mesh):
    placed = (P("tm", "clip", None), P(), P(), P(), P(), P())
    return jax.shard_map(
        functools.partial(body, mesh.shape["tm"]),
        mesh=mesh,
        in_specs=placed,
        out_specs=P(None, ("clip", "tm"), None),
        check_vma=False,
    )
```

```python
import functools

import jax
import jax.numpy as jnp
from jax import lax
from jax.experimental import pallas as pl
from jax.experimental.pallas import tpu as pltpu
from jax.sharding import PartitionSpec as P

ROWS = 4
COLS = 128
MESH = pl.DeviceIdType.MESH


def norm_act(x, gain):
    values = x.astype(jnp.float32)
    scale = lax.rsqrt(jnp.mean(values * values, axis=-1, keepdims=True) + 1e-06)
    scaled = values * scale * gain
    return scaled * (0.5 * jnp.tanh(0.5 * scaled) + 0.5)


def store_shifted(acts, frame, row, act):
    channels = act.shape[-1]
    place = lax.broadcasted_iota(jnp.int32, act.shape, 0)
    before = jnp.where(place == 0, 0.0, pltpu.roll(act, 1, 0))
    after = jnp.where(place == COLS - 1, 0.0, pltpu.roll(act, COLS - 1, 0))
    acts[frame, row, :, :channels] = before.astype(jnp.bfloat16)
    acts[frame, row, :, channels : 2 * channels] = act.astype(jnp.bfloat16)
    acts[frame, row, :, 2 * channels :] = after.astype(jnp.bfloat16)


def conv_row(acts, kernel, frame, source, tap, rows):
    total = None
    for tap_t in range(3):
        for at in range(rows):
            window = acts[pl.ds(frame + tap_t, 2), source + at]
            part = jnp.dot(
                window.reshape(2 * COLS, window.shape[-1]),
                kernel[tap_t * 3 + tap + at],
                preferred_element_type=jnp.float32,
            )
            total = part if total is None else total + part
    return total.reshape(2, COLS, total.shape[-1])


def both_rows(acts, kernel, frame, half):
    border = conv_row(acts, kernel, frame, 2 * half, 1 - half, 2)
    inner = conv_row(acts, kernel, frame, half, 0, 3)
    return (((ROWS - 1) * half, border), (1 + half, inner))


def fused(
    n,
    frames_ref,
    gain_one,
    conv_one,
    gain_two,
    conv_two,
    out_weight,
    out_ref,
    frames,
    halo_one,
    halo_two,
    edge_two,
    kernel_one,
    kernel_two,
    project,
    acts_one,
    acts_two,
    first,
    result,
    load_sems,
    halo_send,
    halo_recv,
    edge_send,
    edge_recv,
    out_send,
    out_recv,
    own_sem,
):
    me = lax.axis_index("tm")
    count = frames.shape[0]
    channels = frames.shape[-1]
    owned = result.shape[2]
    per_row = COLS // owned
    earlier = me - 1
    later = me + 1

    loads = [pltpu.make_async_copy(frames_ref, frames, load_sems.at[0])]
    for source, target in ((conv_one, kernel_one), (conv_two, kernel_two)):
        for tap in range(9):
            sem = load_sems.at[len(loads)]
            loads.append(pltpu.make_async_copy(source.at[tap], target.at[tap], sem))
    loads.append(pltpu.make_async_copy(out_weight, project, load_sems.at[19]))
    for load in loads[:10]:
        load.start()

    barrier = pltpu.get_barrier_semaphore()

    @pl.loop(1, n)
    def _(step):
        pl.semaphore_signal(
            barrier, inc=1, device_id={"tm": lax.rem(me + step, n)}, device_id_type=MESH
        )

    loads[0].wait()

    @pl.loop(0, count * ROWS)
    def _(index):
        frame = index // ROWS
        row = index % ROWS
        act = norm_act(frames[frame, row], gain_one[...])
        store_shifted(acts_one, frame + 2, row, act)

    pl.semaphore_wait(barrier, n - 1)

    halo_copy = pltpu.make_async_remote_copy(
        src_ref=frames_ref.at[pl.ds(count - 2, 2)],
        dst_ref=halo_one,
        send_sem=halo_send,
        recv_sem=halo_recv,
        device_id={"tm": lax.rem(later, n)},
        device_id_type=MESH,
    )

    def edge_copy(row):
        return pltpu.make_async_remote_copy(
            src_ref=edge_two.at[row],
            dst_ref=halo_two.at[row],
            send_sem=edge_send.at[row],
            recv_sem=edge_recv.at[row],
            device_id={"tm": lax.rem(later, n)},
            device_id_type=MESH,
        )

    @pl.when(later < n)
    def _():
        halo_copy.start()

    for load in loads[1:10]:
        load.wait()
    for load in loads[10:]:
        load.start()

    halves = ROWS // 2
    pairs = count // 2
    steps = pairs * halves
    far = 1 - (2 * me) // n

    @pl.loop(0, steps)
    def _(step):
        frame = count - 2 - 2 * (step // halves)
        half = step % halves

        @pl.when((step == steps - halves) & (me > 0))
        def _():
            halo_copy.wait_recv()

            @pl.loop(0, 2 * ROWS)
            def _(index):
                at = index // ROWS
                row = index % ROWS
                store_shifted(acts_one, at, row, norm_act(halo_one[at, row], gain_one[...]))

        @pl.when((step == steps - halves) & (me == 0))
        def _():
            @pl.loop(0, 2 * ROWS)
            def _(index):
                blank = jnp.zeros((COLS, acts_one.shape[-1]), jnp.bfloat16)
                acts_one[index // ROWS, index % ROWS] = blank
                acts_two[index // ROWS, index % ROWS] = blank

        for row, conv in both_rows(acts_one, kernel_one, frame, half):
            for at in range(2):
                value = (frames[frame + at, row].astype(jnp.float32) + conv[at]).astype(
                    jnp.bfloat16
                )
                first[frame + at, row] = value
                store_shifted(acts_two, frame + at + 2, row, norm_act(value, gain_two[...]))

        @pl.when((step < halves) & (later < n))
        def _():
            for row in ((ROWS - 1) * half, 1 + half):
                for at in range(2):
                    edge_two[row, at] = acts_two[count + at, row, :, channels : 2 * channels]
                edge_copy(row).start()

    for load in loads[10:]:
        load.wait()

    @pl.loop(0, steps)
    def _(step):
        frame = count - 2 - 2 * (step % pairs)
        half = (far + step // pairs) % halves

        @pl.when((step == pairs - 1) & (me > 0))
        def _():
            @pl.loop(0, ROWS)
            def _(row):
                edge_copy(row).wait_recv()
                for at in range(2):
                    store_shifted(acts_two, at, row, halo_two[row, at].astype(jnp.float32))

        for row, conv in both_rows(acts_two, kernel_two, frame, half):
            value = (first[pl.ds(frame, 2), row].astype(jnp.float32) + conv).astype(jnp.bfloat16)
            latent = jnp.dot(
                value.reshape(2 * COLS, channels),
                project[...],
                preferred_element_type=jnp.float32,
            ).astype(jnp.bfloat16)
            for at in range(2):
                for index in range(per_row):
                    begin = at * COLS + index * owned
                    result[row * per_row + index, frame + at] = latent[begin : begin + owned]

        for row in ((ROWS - 1) * half, 1 + half):

            @pl.loop(0, per_row)
            def _(index):
                owner = row * per_row + index

                @pl.when(owner != me)
                def _():
                    pltpu.make_async_remote_copy(
                        src_ref=result.at[owner, pl.ds(frame, 2)],
                        dst_ref=out_ref.at[pl.ds(me * count + frame, 2)],
                        send_sem=out_send,
                        recv_sem=out_recv,
                        device_id={"tm": owner},
                        device_id_type=MESH,
                    ).start()

    own = pltpu.make_async_copy(result.at[me], out_ref.at[pl.ds(me * count, count)], own_sem)
    own.start()

    @pl.when(later < n)
    def _():
        halo_copy.wait_send()
        for row in range(ROWS):
            edge_copy(row).wait_send()

    others = out_ref.at[pl.ds(0, (n - 1) * count)]
    sent = result.at[pl.ds(0, n - 1)]
    pltpu.make_async_copy(sent, sent, out_send).wait()
    pltpu.make_async_copy(others, others, out_recv).wait()
    own.wait()


def body(n, frames, gain_one, conv_one, gain_two, conv_two, out_weight):
    count, cells, channels = frames.shape
    owned = cells // n
    grid = (count, ROWS, COLS, channels)
    taps = (9, 3 * channels, channels)
    half = jnp.bfloat16
    hbm = pl.BlockSpec(memory_space=pl.ANY)
    vmem = pl.BlockSpec(memory_space=pltpu.VMEM)
    return pl.pallas_call(
        functools.partial(fused, n),
        out_shape=jax.ShapeDtypeStruct((n * count, owned, channels), half),
        in_specs=[hbm, vmem, hbm, vmem, hbm, hbm],
        out_specs=hbm,
        scratch_shapes=[
            pltpu.VMEM(grid, half),
            pltpu.VMEM((2, ROWS, COLS, channels), half),
            pltpu.VMEM((ROWS, 2, COLS, channels), half),
            pltpu.VMEM((ROWS, 2, COLS, channels), half),
            pltpu.VMEM(taps, half),
            pltpu.VMEM(taps, half),
            pltpu.VMEM((channels, channels), half),
            pltpu.VMEM((count + 2, ROWS, COLS, 3 * channels), half),
            pltpu.VMEM((count + 2, ROWS, COLS, 3 * channels), half),
            pltpu.VMEM(grid, half),
            pltpu.VMEM((n, count, owned, channels), half),
            pltpu.SemaphoreType.DMA((20,)),
            pltpu.SemaphoreType.DMA,
            pltpu.SemaphoreType.DMA,
            pltpu.SemaphoreType.DMA((ROWS,)),
            pltpu.SemaphoreType.DMA((ROWS,)),
            pltpu.SemaphoreType.DMA,
            pltpu.SemaphoreType.DMA,
            pltpu.SemaphoreType.DMA,
        ],
        compiler_params=pltpu.CompilerParams(collective_id=0, has_side_effects=True),
    )(
        frames.reshape(grid),
        gain_one.reshape(1, channels),
        conv_one.reshape(taps),
        gain_two.reshape(1, channels),
        conv_two.reshape(taps),
        out_weight,
    )


def solution(mesh):
    placed = (P("tm", "clip", None), P(), P(), P(), P(), P())
    return jax.shard_map(
        functools.partial(body, mesh.shape["tm"]),
        mesh=mesh,
        in_specs=placed,
        out_specs=P(None, ("clip", "tm"), None),
        check_vma=False,
    )
```

```python
import functools

import jax
import jax.numpy as jnp
from jax import lax
from jax.experimental import pallas as pl
from jax.experimental.pallas import tpu as pltpu
from jax.sharding import PartitionSpec as P

ROWS = 4
COLS = 128
MESH = pl.DeviceIdType.MESH


def norm_act(x, gain):
    values = x.astype(jnp.float32)
    scale = lax.rsqrt(jnp.mean(values * values, axis=-1, keepdims=True) + 1e-06)
    scaled = values * scale * gain
    return scaled * (0.5 * jnp.tanh(0.5 * scaled) + 0.5)


def store_shifted(acts, frame, row, act):
    channels = act.shape[-1]
    place = lax.broadcasted_iota(jnp.int32, act.shape, 0)
    before = jnp.where(place == 0, 0.0, pltpu.roll(act, 1, 0))
    after = jnp.where(place == COLS - 1, 0.0, pltpu.roll(act, COLS - 1, 0))
    acts[frame, row, :, :channels] = before.astype(jnp.bfloat16)
    acts[frame, row, :, channels : 2 * channels] = act.astype(jnp.bfloat16)
    acts[frame, row, :, 2 * channels :] = after.astype(jnp.bfloat16)


def conv_row(acts, kernel, frame, source, tap, rows):
    total = None
    for tap_t in range(3):
        for at in range(rows):
            window = acts[pl.ds(frame + tap_t, 2), source + at]
            part = jnp.dot(
                window.reshape(2 * COLS, window.shape[-1]),
                kernel[tap_t * 3 + tap + at],
                preferred_element_type=jnp.float32,
            )
            total = part if total is None else total + part
    return total.reshape(2, COLS, total.shape[-1])


def both_rows(acts, kernel, frame, half):
    border = conv_row(acts, kernel, frame, 2 * half, 1 - half, 2)
    inner = conv_row(acts, kernel, frame, half, 0, 3)
    return (((ROWS - 1) * half, border), (1 + half, inner))


def fused(
    n,
    frames_ref,
    gain_one,
    conv_one,
    gain_two,
    conv_two,
    out_weight,
    out_ref,
    frames,
    halo_one,
    halo_two,
    edge_two,
    kernel_one,
    kernel_two,
    project,
    acts_one,
    acts_two,
    first,
    result,
    load_sems,
    halo_send,
    halo_recv,
    edge_send,
    edge_recv,
    out_send,
    out_recv,
    own_sem,
):
    me = lax.axis_index("tm")
    count = frames.shape[0]
    channels = frames.shape[-1]
    owned = result.shape[2]
    per_row = COLS // owned
    earlier = me - 1
    later = me + 1

    loads = [pltpu.make_async_copy(frames_ref, frames, load_sems.at[0])]
    for source, target in ((conv_one, kernel_one), (conv_two, kernel_two)):
        for tap in range(9):
            sem = load_sems.at[len(loads)]
            loads.append(pltpu.make_async_copy(source.at[tap], target.at[tap], sem))
    loads.append(pltpu.make_async_copy(out_weight, project, load_sems.at[19]))
    for load in loads[:10]:
        load.start()

    barrier = pltpu.get_barrier_semaphore()

    @pl.loop(1, n)
    def _(step):
        pl.semaphore_signal(
            barrier, inc=1, device_id={"tm": lax.rem(me + step, n)}, device_id_type=MESH
        )

    loads[0].wait()

    @pl.loop(0, count * ROWS)
    def _(index):
        frame = index // ROWS
        row = index % ROWS
        act = norm_act(frames[frame, row], gain_one[...])
        store_shifted(acts_one, frame + 2, row, act)

    pl.semaphore_wait(barrier, n - 1)

    halo_copy = pltpu.make_async_remote_copy(
        src_ref=frames_ref.at[pl.ds(count - 2, 2)],
        dst_ref=halo_one,
        send_sem=halo_send,
        recv_sem=halo_recv,
        device_id={"tm": lax.rem(later, n)},
        device_id_type=MESH,
    )

    def edge_copy(row):
        return pltpu.make_async_remote_copy(
            src_ref=edge_two.at[row],
            dst_ref=halo_two.at[row],
            send_sem=edge_send.at[row],
            recv_sem=edge_recv.at[row],
            device_id={"tm": lax.rem(later, n)},
            device_id_type=MESH,
        )

    @pl.when(later < n)
    def _():
        halo_copy.start()

    for load in loads[1:10]:
        load.wait()
    for load in loads[10:]:
        load.start()

    halves = ROWS // 2
    pairs = count // 2
    far = 1 - (2 * me) // n

    def finish(frame, row, conv):
        value = (first[pl.ds(frame, 2), row].astype(jnp.float32) + conv).astype(jnp.bfloat16)
        latent = jnp.dot(
            value.reshape(2 * COLS, channels),
            project[...],
            preferred_element_type=jnp.float32,
        ).astype(jnp.bfloat16)
        for at in range(2):
            for index in range(per_row):
                begin = at * COLS + index * owned
                result[row * per_row + index, frame + at] = latent[begin : begin + owned]

    @pl.loop(0, halves)
    def _(stage):
        near = (far + stage) % halves

        @pl.loop(0, pairs)
        def _(step):
            frame = count - 2 - 2 * step
            head = (stage == 0) & (step == pairs - 1)

            @pl.when(head & (me > 0))
            def _():
                halo_copy.wait_recv()

                @pl.loop(0, 2 * ROWS)
                def _(index):
                    at = index // ROWS
                    row = index % ROWS
                    store_shifted(acts_one, at, row, norm_act(halo_one[at, row], gain_one[...]))

            @pl.when(head & (me == 0))
            def _():
                @pl.loop(0, 2 * ROWS)
                def _(index):
                    blank = jnp.zeros((COLS, acts_one.shape[-1]), jnp.bfloat16)
                    acts_one[index // ROWS, index % ROWS] = blank
                    acts_two[index // ROWS, index % ROWS] = blank

            for row, conv in both_rows(acts_one, kernel_one, frame, near):
                for at in range(2):
                    value = (frames[frame + at, row].astype(jnp.float32) + conv[at]).astype(
                        jnp.bfloat16
                    )
                    first[frame + at, row] = value
                    store_shifted(acts_two, frame + at + 2, row, norm_act(value, gain_two[...]))

            @pl.when((step == 0) & (later < n))
            def _():
                for row in ((ROWS - 1) * near, 1 + near):
                    for at in range(2):
                        edge_two[row, at] = acts_two[count + at, row, :, channels : 2 * channels]
                    edge_copy(row).start()

        @pl.when(stage == 0)
        def _():
            for load in loads[10:]:
                load.wait()

        @pl.loop(stage * pairs, (3 * stage + 1) * pairs)
        def _(step):
            unit = step // pairs
            frame = count - 2 - 2 * (step % pairs)
            half = (far + unit // 2) % halves
            inner = unit % 2

            @pl.when((unit < 2) & (frame == 0) & (me > 0))
            def _():
                @pl.loop(0, 2)
                def _(index):
                    row = 2 * near + index
                    edge_copy(row).wait_recv()
                    for at in range(2):
                        store_shifted(acts_two, at, row, halo_two[row, at].astype(jnp.float32))

            @pl.when(inner == 0)
            def _():
                conv = conv_row(acts_two, kernel_two, frame, 2 * half, 1 - half, 2)
                finish(frame, (ROWS - 1) * half, conv)

            @pl.when(inner == 1)
            def _():
                finish(frame, 1 + half, conv_row(acts_two, kernel_two, frame, half, 0, 3))

            row = 2 * half + (half + inner) % 2

            @pl.loop(0, per_row)
            def _(index):
                owner = row * per_row + index

                @pl.when(owner != me)
                def _():
                    pltpu.make_async_remote_copy(
                        src_ref=result.at[owner, pl.ds(frame, 2)],
                        dst_ref=out_ref.at[pl.ds(me * count + frame, 2)],
                        send_sem=out_send,
                        recv_sem=out_recv,
                        device_id={"tm": owner},
                        device_id_type=MESH,
                    ).start()

    own = pltpu.make_async_copy(result.at[me], out_ref.at[pl.ds(me * count, count)], own_sem)
    own.start()

    @pl.when(later < n)
    def _():
        halo_copy.wait_send()
        for row in range(ROWS):
            edge_copy(row).wait_send()

    others = out_ref.at[pl.ds(0, (n - 1) * count)]
    sent = result.at[pl.ds(0, n - 1)]
    pltpu.make_async_copy(sent, sent, out_send).wait()
    pltpu.make_async_copy(others, others, out_recv).wait()
    own.wait()


def body(n, frames, gain_one, conv_one, gain_two, conv_two, out_weight):
    count, cells, channels = frames.shape
    owned = cells // n
    grid = (count, ROWS, COLS, channels)
    taps = (9, 3 * channels, channels)
    half = jnp.bfloat16
    hbm = pl.BlockSpec(memory_space=pl.ANY)
    vmem = pl.BlockSpec(memory_space=pltpu.VMEM)
    return pl.pallas_call(
        functools.partial(fused, n),
        out_shape=jax.ShapeDtypeStruct((n * count, owned, channels), half),
        in_specs=[hbm, vmem, hbm, vmem, hbm, hbm],
        out_specs=hbm,
        scratch_shapes=[
            pltpu.VMEM(grid, half),
            pltpu.VMEM((2, ROWS, COLS, channels), half),
            pltpu.VMEM((ROWS, 2, COLS, channels), half),
            pltpu.VMEM((ROWS, 2, COLS, channels), half),
            pltpu.VMEM(taps, half),
            pltpu.VMEM(taps, half),
            pltpu.VMEM((channels, channels), half),
            pltpu.VMEM((count + 2, ROWS, COLS, 3 * channels), half),
            pltpu.VMEM((count + 2, ROWS, COLS, 3 * channels), half),
            pltpu.VMEM(grid, half),
            pltpu.VMEM((n, count, owned, channels), half),
            pltpu.SemaphoreType.DMA((20,)),
            pltpu.SemaphoreType.DMA,
            pltpu.SemaphoreType.DMA,
            pltpu.SemaphoreType.DMA((ROWS,)),
            pltpu.SemaphoreType.DMA((ROWS,)),
            pltpu.SemaphoreType.DMA,
            pltpu.SemaphoreType.DMA,
            pltpu.SemaphoreType.DMA,
        ],
        compiler_params=pltpu.CompilerParams(collective_id=0, has_side_effects=True),
    )(
        frames.reshape(grid),
        gain_one.reshape(1, channels),
        conv_one.reshape(taps),
        gain_two.reshape(1, channels),
        conv_two.reshape(taps),
        out_weight,
    )


def solution(mesh):
    placed = (P("tm", "clip", None), P(), P(), P(), P(), P())
    return jax.shard_map(
        functools.partial(body, mesh.shape["tm"]),
        mesh=mesh,
        in_specs=placed,
        out_specs=P(None, ("clip", "tm"), None),
        check_vma=False,
    )
```

```python
import functools

import jax
import jax.numpy as jnp
from jax import lax
from jax.experimental import pallas as pl
from jax.experimental.pallas import tpu as pltpu
from jax.sharding import PartitionSpec as P

ROWS = 4
COLS = 128
MESH = pl.DeviceIdType.MESH


def norm_act(x, gain):
    values = x.astype(jnp.float32)
    scale = lax.rsqrt(jnp.mean(values * values, axis=-1, keepdims=True) + 1e-06)
    scaled = values * scale * gain
    return scaled * (0.5 * jnp.tanh(0.5 * scaled) + 0.5)


def store_shifted(acts, frame, row, act):
    channels = act.shape[-1]
    place = lax.broadcasted_iota(jnp.int32, act.shape, 0)
    before = jnp.where(place == 0, 0.0, pltpu.roll(act, 1, 0))
    after = jnp.where(place == COLS - 1, 0.0, pltpu.roll(act, COLS - 1, 0))
    acts[frame, row, :, :channels] = before.astype(jnp.bfloat16)
    acts[frame, row, :, channels : 2 * channels] = act.astype(jnp.bfloat16)
    acts[frame, row, :, 2 * channels :] = after.astype(jnp.bfloat16)


def conv_row(acts, kernel, frame, source, tap, rows):
    total = None
    for tap_t in range(3):
        for at in range(rows):
            window = acts[pl.ds(frame + tap_t, 2), source + at]
            part = jnp.dot(
                window.reshape(2 * COLS, window.shape[-1]),
                kernel[tap_t * 3 + tap + at],
                preferred_element_type=jnp.float32,
            )
            total = part if total is None else total + part
    return total.reshape(2, COLS, total.shape[-1])


def both_rows(acts, kernel, frame, half):
    border = conv_row(acts, kernel, frame, 2 * half, 1 - half, 2)
    inner = conv_row(acts, kernel, frame, half, 0, 3)
    return (((ROWS - 1) * half, border), (1 + half, inner))


def fused(
    n,
    frames_ref,
    gain_one,
    conv_one,
    gain_two,
    conv_two,
    out_weight,
    out_ref,
    frames,
    halo_one,
    halo_two,
    edge_two,
    kernel_one,
    kernel_two,
    project,
    acts_one,
    acts_two,
    first,
    result,
    load_sems,
    halo_send,
    halo_recv,
    edge_send,
    edge_recv,
    out_send,
    out_recv,
    own_sem,
):
    me = lax.axis_index("tm")
    count = frames.shape[0]
    channels = frames.shape[-1]
    owned = result.shape[2]
    per_row = COLS // owned
    earlier = me - 1
    later = me + 1

    loads = [pltpu.make_async_copy(frames_ref, frames, load_sems.at[0])]
    for source, target in ((conv_one, kernel_one), (conv_two, kernel_two)):
        for tap in range(9):
            sem = load_sems.at[len(loads)]
            loads.append(pltpu.make_async_copy(source.at[tap], target.at[tap], sem))
    loads.append(pltpu.make_async_copy(out_weight, project, load_sems.at[19]))
    for load in loads[:10]:
        load.start()

    barrier = pltpu.get_barrier_semaphore()

    @pl.loop(1, n)
    def _(step):
        pl.semaphore_signal(
            barrier, inc=1, device_id={"tm": lax.rem(me + step, n)}, device_id_type=MESH
        )

    loads[0].wait()

    @pl.loop(0, count * ROWS)
    def _(index):
        frame = index // ROWS
        row = index % ROWS
        act = norm_act(frames[frame, row], gain_one[...])
        store_shifted(acts_one, frame + 2, row, act)

    pl.semaphore_wait(barrier, n - 1)

    halo_copy = pltpu.make_async_remote_copy(
        src_ref=frames_ref.at[pl.ds(count - 2, 2)],
        dst_ref=halo_one,
        send_sem=halo_send,
        recv_sem=halo_recv,
        device_id={"tm": lax.rem(later, n)},
        device_id_type=MESH,
    )

    def edge_copy(row):
        return pltpu.make_async_remote_copy(
            src_ref=edge_two.at[row],
            dst_ref=halo_two.at[row],
            send_sem=edge_send.at[row],
            recv_sem=edge_recv.at[row],
            device_id={"tm": lax.rem(later, n)},
            device_id_type=MESH,
        )

    @pl.when(later < n)
    def _():
        halo_copy.start()

    for load in loads[1:10]:
        load.wait()
    for load in loads[10:]:
        load.start()

    halves = ROWS // 2
    pairs = count // 2
    steps = pairs * halves
    far = 1 - (2 * me) // n

    def finish(frame, row, conv):
        value = (first[pl.ds(frame, 2), row].astype(jnp.float32) + conv).astype(jnp.bfloat16)
        latent = jnp.dot(
            value.reshape(2 * COLS, channels),
            project[...],
            preferred_element_type=jnp.float32,
        ).astype(jnp.bfloat16)
        for at in range(2):
            for index in range(per_row):
                begin = at * COLS + index * owned
                result[row * per_row + index, frame + at] = latent[begin : begin + owned]

    @pl.loop(0, halves)
    def _(stage):

        @pl.loop(stage * (steps - 1), steps - 1 + stage)
        def _(step):
            frame = count - 2 - 2 * (step // halves)
            near = (far + step) % halves
            head = step == steps - halves

            @pl.when(head & (me > 0))
            def _():
                halo_copy.wait_recv()

                @pl.loop(0, 2 * ROWS)
                def _(index):
                    at = index // ROWS
                    row = index % ROWS
                    store_shifted(acts_one, at, row, norm_act(halo_one[at, row], gain_one[...]))

            @pl.when(head & (me == 0))
            def _():
                @pl.loop(0, 2 * ROWS)
                def _(index):
                    blank = jnp.zeros((COLS, acts_one.shape[-1]), jnp.bfloat16)
                    acts_one[index // ROWS, index % ROWS] = blank
                    acts_two[index // ROWS, index % ROWS] = blank

            for row, conv in both_rows(acts_one, kernel_one, frame, near):
                for at in range(2):
                    value = (frames[frame + at, row].astype(jnp.float32) + conv[at]).astype(
                        jnp.bfloat16
                    )
                    first[frame + at, row] = value
                    store_shifted(acts_two, frame + at + 2, row, norm_act(value, gain_two[...]))

            @pl.when((step < halves) & (later < n))
            def _():
                for row in ((ROWS - 1) * near, 1 + near):
                    for at in range(2):
                        edge_two[row, at] = acts_two[count + at, row, :, channels : 2 * channels]
                    edge_copy(row).start()

        @pl.when(stage == 0)
        def _():
            for load in loads[10:]:
                load.wait()

        @pl.loop(stage * pairs, (3 * stage + 1) * pairs)
        def _(step):
            unit = step // pairs
            frame = count - 2 - 2 * (step % pairs)
            half = (far + unit // 2) % halves
            inner = unit % 2

            @pl.when((step == pairs - 1) & (me > 0))
            def _():
                @pl.loop(0, ROWS)
                def _(row):
                    edge_copy(row).wait_recv()
                    for at in range(2):
                        store_shifted(acts_two, at, row, halo_two[row, at].astype(jnp.float32))

            @pl.when(inner == 0)
            def _():
                conv = conv_row(acts_two, kernel_two, frame, 2 * half, 1 - half, 2)
                finish(frame, (ROWS - 1) * half, conv)

            @pl.when(inner == 1)
            def _():
                finish(frame, 1 + half, conv_row(acts_two, kernel_two, frame, half, 0, 3))

            row = 2 * half + (half + inner) % 2

            @pl.loop(0, per_row)
            def _(index):
                owner = row * per_row + index

                @pl.when(owner != me)
                def _():
                    pltpu.make_async_remote_copy(
                        src_ref=result.at[owner, pl.ds(frame, 2)],
                        dst_ref=out_ref.at[pl.ds(me * count + frame, 2)],
                        send_sem=out_send,
                        recv_sem=out_recv,
                        device_id={"tm": owner},
                        device_id_type=MESH,
                    ).start()

    own = pltpu.make_async_copy(result.at[me], out_ref.at[pl.ds(me * count, count)], own_sem)
    own.start()

    @pl.when(later < n)
    def _():
        halo_copy.wait_send()
        for row in range(ROWS):
            edge_copy(row).wait_send()

    others = out_ref.at[pl.ds(0, (n - 1) * count)]
    sent = result.at[pl.ds(0, n - 1)]
    pltpu.make_async_copy(sent, sent, out_send).wait()
    pltpu.make_async_copy(others, others, out_recv).wait()
    own.wait()


def body(n, frames, gain_one, conv_one, gain_two, conv_two, out_weight):
    count, cells, channels = frames.shape
    owned = cells // n
    grid = (count, ROWS, COLS, channels)
    taps = (9, 3 * channels, channels)
    half = jnp.bfloat16
    hbm = pl.BlockSpec(memory_space=pl.ANY)
    vmem = pl.BlockSpec(memory_space=pltpu.VMEM)
    return pl.pallas_call(
        functools.partial(fused, n),
        out_shape=jax.ShapeDtypeStruct((n * count, owned, channels), half),
        in_specs=[hbm, vmem, hbm, vmem, hbm, hbm],
        out_specs=hbm,
        scratch_shapes=[
            pltpu.VMEM(grid, half),
            pltpu.VMEM((2, ROWS, COLS, channels), half),
            pltpu.VMEM((ROWS, 2, COLS, channels), half),
            pltpu.VMEM((ROWS, 2, COLS, channels), half),
            pltpu.VMEM(taps, half),
            pltpu.VMEM(taps, half),
            pltpu.VMEM((channels, channels), half),
            pltpu.VMEM((count + 2, ROWS, COLS, 3 * channels), half),
            pltpu.VMEM((count + 2, ROWS, COLS, 3 * channels), half),
            pltpu.VMEM(grid, half),
            pltpu.VMEM((n, count, owned, channels), half),
            pltpu.SemaphoreType.DMA((20,)),
            pltpu.SemaphoreType.DMA,
            pltpu.SemaphoreType.DMA,
            pltpu.SemaphoreType.DMA((ROWS,)),
            pltpu.SemaphoreType.DMA((ROWS,)),
            pltpu.SemaphoreType.DMA,
            pltpu.SemaphoreType.DMA,
            pltpu.SemaphoreType.DMA,
        ],
        compiler_params=pltpu.CompilerParams(collective_id=0, has_side_effects=True),
    )(
        frames.reshape(grid),
        gain_one.reshape(1, channels),
        conv_one.reshape(taps),
        gain_two.reshape(1, channels),
        conv_two.reshape(taps),
        out_weight,
    )


def solution(mesh):
    placed = (P("tm", "clip", None), P(), P(), P(), P(), P())
    return jax.shard_map(
        functools.partial(body, mesh.shape["tm"]),
        mesh=mesh,
        in_specs=placed,
        out_specs=P(None, ("clip", "tm"), None),
        check_vma=False,
    )
```
